32 devices in a mesh: dp: 1 (over z), tp: 4 (over y), cp: 8 (over x, core).
Axes of the slice: x: 4, y: 4, z: 1, core: 2. Of those that a mesh axis runs over, the one named last changes fastest.
The devices are a block of a 4x4x8 slice.
Arguments:
- hidden: bfloat16 [2048, 8192], P(('dp', 'cp'))
- tok_pos: int32 [2048], P(('dp', 'cp'))
- norm_gain: float32 [8192], replicated
- w_query: bfloat16 [8192, 8192], P(None, 'tp')
- w_key: bfloat16 [8192, 1024], P(None, 'tp')
- w_value: bfloat16 [8192, 1024], P(None, 'tp')
- w_out: bfloat16 [8192, 8192], P('tp')
Outputs:
- output 1: bfloat16 [2048, 8192], P(('dp', 'cp'))
- output 2: bfloat16 [2048, 8, 128], P(('dp', 'cp'), 'tp')
- output 3: bfloat16 [2048, 8, 128], P(('dp', 'cp'), 'tp')
All inputs are finite; a program needn't handle non-finite values.
Results may differ from the reference program's by a relative error of at most 0.00490248.
Values are sent between devices in bfloat16 or wider.
A program may use at most 768 MiB of HBM per device.

```python
import math
import jax
import jax.numpy as jnp
from jax import lax

D = 8192
HEADS = 64
KV_HEADS = 8
HEAD = 128
SEQ = 2048
RUN_LEN = 128
Q_BLOCK = 128
THETA = 1000000
EPS = 1e-5


def setup_inputs(seed: int = 0, part: int = 0) -> dict:
    shared = jax.random.split(jax.random.key(seed), 5)
    local = jax.random.split(jax.random.fold_in(jax.random.key(seed + 1), part), 4)
    run_order = jax.random.permutation(local[0], SEQ // RUN_LEN)
    tok_pos = (run_order[:, None] * RUN_LEN + jnp.arange(RUN_LEN)[None, :]).reshape(SEQ).astype(jnp.int32)
    waves = jax.random.normal(local[1], (4, D), jnp.float32)
    phases = jax.random.uniform(local[2], (4,), jnp.float32, 0.0, 2.0 * math.pi)
    cycles = jnp.array([0.5, 1.0, 1.5, 2.5], jnp.float32)
    angle = tok_pos.astype(jnp.float32)[:, None] * (cycles * (2.0 * math.pi / SEQ))[None, :] + phases[None, :]
    signal = jnp.dot(jnp.cos(angle), waves)
    noise = jax.random.normal(local[3], (SEQ, D), jnp.float32)
    hidden = (0.25 * signal + 0.2 * noise).astype(jnp.bfloat16)
    norm_gain = 1.0 + 0.3 * jax.random.normal(shared[0], (D,), jnp.float32)
    w_query = (jax.random.normal(shared[1], (D, HEADS * HEAD), jnp.float32) * D ** -0.5).astype(jnp.bfloat16)
    w_key = (jax.random.normal(shared[2], (D, KV_HEADS * HEAD), jnp.float32) * D ** -0.5).astype(jnp.bfloat16)
    w_value = (jax.random.normal(shared[3], (D, KV_HEADS * HEAD), jnp.float32) * D ** -0.5).astype(jnp.bfloat16)
    w_out = (jax.random.normal(shared[4], (HEADS * HEAD, D), jnp.float32) * (HEADS * HEAD) ** -0.5).astype(jnp.bfloat16)
    return {"hidden": hidden, "tok_pos": tok_pos, "norm_gain": norm_gain, "w_query": w_query, "w_key": w_key, "w_value": w_value, "w_out": w_out}


def rope_tables(tok_pos):
    inv_freq = 1.0 / (THETA ** (jnp.arange(0, HEAD, 2, dtype=jnp.float32) / HEAD))
    angles = tok_pos.astype(jnp.float32)[:, None] * inv_freq[None, :]
    return jnp.cos(angles)[:, None, :], jnp.sin(angles)[:, None, :]


def rotate_half(head_vecs, cos_tab, sin_tab):
    half_dim = head_vecs.shape[-1] // 2
    first_half = head_vecs[..., :half_dim].astype(jnp.float32)
    second_half = head_vecs[..., half_dim:].astype(jnp.float32)
    rotated = jnp.concatenate([first_half * cos_tab - second_half * sin_tab, second_half * cos_tab + first_half * sin_tab], axis=-1)
    return rotated.astype(jnp.bfloat16)


def reference(hidden, tok_pos, norm_gain, w_query, w_key, w_value, w_out):
    q_per_kv = HEADS // KV_HEADS
    n_blocks = SEQ // Q_BLOCK
    hid_f32 = hidden.astype(jnp.float32)
    normed = (hid_f32 * lax.rsqrt(jnp.mean(hid_f32 * hid_f32, axis=-1, keepdims=True) + EPS) * norm_gain).astype(jnp.bfloat16)
    queries = jnp.dot(normed, w_query, preferred_element_type=jnp.float32).astype(jnp.bfloat16).reshape(SEQ, HEADS, HEAD)
    keys_raw = jnp.dot(normed, w_key, preferred_element_type=jnp.float32).astype(jnp.bfloat16).reshape(SEQ, KV_HEADS, HEAD)
    values = jnp.dot(normed, w_value, preferred_element_type=jnp.float32).astype(jnp.bfloat16).reshape(SEQ, KV_HEADS, HEAD)
    cos_tab, sin_tab = rope_tables(tok_pos)
    q_rot = rotate_half(queries, cos_tab, sin_tab)
    k_rot = rotate_half(keys_raw, cos_tab, sin_tab)
    attn_scale = HEAD ** -0.5
    k_heads = jnp.transpose(k_rot, (1, 0, 2)).astype(jnp.float32)
    v_heads = jnp.transpose(values, (1, 0, 2)).astype(jnp.float32)
    q_blocks = jnp.transpose(q_rot.reshape(n_blocks, Q_BLOCK, KV_HEADS, q_per_kv, HEAD), (0, 2, 1, 3, 4))
    pos_blocks = tok_pos.reshape(n_blocks, Q_BLOCK)

    def one_block(block_in):
        q_blk, pos_blk = block_in
        allowed = tok_pos[None, :] <= pos_blk[:, None]

        def one_head(head_in):
            q_head, k_head, v_head = head_in
            scores = jnp.einsum("qgd,td->gqt", q_head.astype(jnp.float32), k_head) * attn_scale
            scores = jnp.where(allowed[None], scores, -jnp.inf)
            softmaxed = jax.nn.softmax(scores, axis=-1)
            return jnp.einsum("gqt,td->qgd", softmaxed, v_head)

        return lax.map(one_head, (q_blk, k_heads, v_heads))

    context = lax.map(one_block, (q_blocks, pos_blocks))
    attn_out = jnp.transpose(context, (0, 2, 1, 3, 4)).reshape(SEQ, HEADS * HEAD).astype(jnp.bfloat16)
    attn_proj = jnp.dot(attn_out, w_out, preferred_element_type=jnp.float32)
    return (hid_f32 + attn_proj).astype(jnp.bfloat16), k_rot, values
```

```python
import functools
import math

import jax
import jax.numpy as jnp
from jax import lax
from jax.experimental import pallas as pl
from jax.experimental.pallas import tpu as pltpu
from jax.sharding import PartitionSpec as P

HEAD = 128
THETA = 1000000
EPS = 1e-5
MESH = pl.DeviceIdType.MESH
BLOCKS = 4
STACK = 4
OPP, PREV, NEXT, OWN = 0, 1, 2, 3


def rms_normed(hid_f32, norm_gain):
    scaled = hid_f32 * lax.rsqrt(jnp.mean(hid_f32 * hid_f32, axis=-1, keepdims=True) + EPS)
    return (scaled * norm_gain).astype(jnp.bfloat16)


def rope_tables(tok_pos):
    inv_freq = 1.0 / (THETA ** (jnp.arange(0, HEAD, 2, dtype=jnp.float32) / HEAD))
    angles = tok_pos.astype(jnp.float32)[:, None] * inv_freq[None, :]
    return jnp.cos(angles)[:, None, :], jnp.sin(angles)[:, None, :]


def rotate_half(head_vecs, cos_tab, sin_tab):
    half_dim = head_vecs.shape[-1] // 2
    first_half = head_vecs[..., :half_dim].astype(jnp.float32)
    second_half = head_vecs[..., half_dim:].astype(jnp.float32)
    rotated = jnp.concatenate([first_half * cos_tab - second_half * sin_tab, second_half * cos_tab + first_half * sin_tab], axis=-1)
    return rotated.astype(jnp.bfloat16)


def mix_kernel(
    n,
    q_ref, k_ref, v_ref, posq_ref, posk_ref, x_hbm, w_hbm, out_hbm,
    w_ref, x_ref, bias_ref, o_ref,
    opp_send, opp_recv, side_send, side_recv, side_part, own_part, own_out, fwd_recv,
    w_sem, x_sem, out_sem, opp_ssem, opp_rsem, side_ssem, side_rsem, ag_ssem, ag_rsem, fwd_ssem, fwd_rsem,
):
    heads, rows, _ = q_ref.shape
    seq, kv_cols = k_ref.shape
    q_per_kv = heads // (kv_cols // HEAD)
    width = w_hbm.shape[1]
    chunk = width // n
    half = chunk // 2
    blk = rows // BLOCKS
    coef = HEAD ** -0.5 * math.log2(math.e)

    me = lax.axis_index("tp")
    right, left = lax.rem(me + 1, n), lax.rem(me + n - 1, n)
    owners = (lax.rem(me + 2, n), left, right, me)

    def w_copy(idx):
        col = pl.multiple_of(owners[idx // 2] * chunk + (idx % 2) * half, half)
        return pltpu.make_async_copy(w_hbm.at[:, pl.ds(col, half)], w_ref.at[idx], w_sem.at[idx])

    x_copy = pltpu.make_async_copy(x_hbm.at[:, pl.ds(pl.multiple_of(me * chunk, chunk), chunk)], x_ref, x_sem)

    for idx in (0, 1, 3, 4, 2, 5, 6, 7):
        w_copy(idx).start()
    x_copy.start()

    barrier = pltpu.get_barrier_semaphore()
    for side in (left, right):
        pl.semaphore_signal(barrier, inc=1, device_id={"tp": side}, device_id_type=MESH)
    pl.semaphore_wait(barrier, 2)

    sides = (left, right)

    def opp_copy(b, s):
        return pltpu.make_async_remote_copy(
            src_ref=opp_send.at[b, s], dst_ref=opp_recv.at[b, s], send_sem=opp_ssem.at[b, s], recv_sem=opp_rsem.at[b, s],
            device_id={"tp": sides[s]}, device_id_type=MESH)

    def side_copy(b, s, h):
        return pltpu.make_async_remote_copy(
            src_ref=side_send.at[b, s, h], dst_ref=side_recv.at[b, s, h], send_sem=side_ssem.at[b, s, h],
            recv_sem=side_rsem.at[b, s, h], device_id={"tp": sides[s]}, device_id_type=MESH)

    def out_at(b, owner, h):
        row = pl.multiple_of(b * blk, blk)
        col = pl.multiple_of(owner * chunk + h * half, half)
        return out_hbm.at[pl.ds(row, blk), pl.ds(col, half)]

    def ag_copy(b, s, h):
        hands_on = h == (0 if s == 1 else 1)
        dst = fwd_recv.at[b, s] if hands_on else out_at(b, me, h)
        return pltpu.make_async_remote_copy(
            src_ref=own_out.at[b, h], dst_ref=dst, send_sem=ag_ssem.at[b, s, h], recv_sem=ag_rsem.at[b, s, h],
            device_id={"tp": sides[s]}, device_id_type=MESH)

    def fwd_copy(b, s):
        owner, h = (left, 0) if s == 1 else (right, 1)
        return pltpu.make_async_remote_copy(
            src_ref=fwd_recv.at[b, s], dst_ref=out_at(b, owner, h), send_sem=fwd_ssem.at[b, s], recv_sem=fwd_rsem.at[b, s],
            device_id={"tp": sides[s]}, device_id_type=MESH)

    def own_store(b, h):
        return pltpu.make_async_copy(own_out.at[b, h], out_at(b, me, h), out_sem.at[b, h])

    def fwd_store(b, s):
        owner, h = (left, 0) if s == 1 else (right, 1)
        return pltpu.make_async_copy(fwd_recv.at[b, s], out_at(b, owner, h), out_sem.at[b, 2 + s])

    def attention(b):
        row = pl.multiple_of(b * blk, blk)
        bias_ref[...] = jnp.where(posk_ref[...] <= posq_ref[pl.ds(row, blk), :], 0.0, -jnp.inf)

        def heads_step(i, carry):
            first = i * STACK
            kv = pl.multiple_of((first // q_per_kv) * HEAD, HEAD)
            q = q_ref[pl.ds(first, STACK), pl.ds(row, blk), :].reshape(STACK * blk, HEAD)
            s = lax.dot_general(q, k_ref[:, pl.ds(kv, HEAD)], (((1,), (1,)), ((), ())), preferred_element_type=jnp.float32)
            s = (s * coef).reshape(STACK, blk, seq) + bias_ref[...][None]
            s = s.reshape(STACK * blk, seq)
            p = jnp.exp2(s - jnp.max(s, axis=-1, keepdims=True))
            total = jnp.sum(p, axis=-1, keepdims=True)
            o = jnp.dot(p.astype(jnp.bfloat16), v_ref[:, pl.ds(kv, HEAD)], preferred_element_type=jnp.float32)
            o = (o / total).astype(jnp.bfloat16)
            for h in range(STACK):
                o_ref[:, pl.ds(pl.multiple_of((first + h) * HEAD, HEAD), HEAD)] = o[h * blk:(h + 1) * blk]
            return carry

        lax.fori_loop(0, heads // STACK, heads_step, 0)

    def project(b):
        def part(idx):
            @pl.when(b == 0)
            def _():
                w_copy(idx).wait()
            return jnp.dot(o_ref[...], w_ref[idx], preferred_element_type=jnp.float32)

        opp_send[b, 0] = part(0).astype(jnp.bfloat16)
        opp_copy(b, 0).start()
        opp_send[b, 1] = part(1).astype(jnp.bfloat16)
        opp_copy(b, 1).start()
        side_send[b, 0, 1] = part(2 * PREV + 1).astype(jnp.bfloat16)
        side_copy(b, 0, 1).start()
        side_send[b, 1, 0] = part(2 * NEXT).astype(jnp.bfloat16)
        side_copy(b, 1, 0).start()
        side_part[b, 0] = part(2 * PREV)
        side_part[b, 1] = part(2 * NEXT + 1)
        for h in range(2):
            own_part[b, h] = part(2 * OWN + h)

    def pass_on(b):
        for s in range(2):
            opp_copy(b, s).wait_recv()
            side_send[b, s, s] = (side_part[b, s] + opp_recv[b, s].astype(jnp.float32)).astype(jnp.bfloat16)
            side_copy(b, s, s).start()

    def finish(b):
        row = pl.multiple_of(b * blk, blk)

        @pl.when(b == 0)
        def _():
            x_copy.wait()

        for h in range(2):
            for s in range(2):
                side_copy(b, s, h).wait_recv()
            total = own_part[b, h] + side_recv[b, 0, h].astype(jnp.float32) + side_recv[b, 1, h].astype(jnp.float32)
            x = x_ref[pl.ds(row, blk), h * half:(h + 1) * half].astype(jnp.float32)
            own_out[b, h] = (x + total).astype(jnp.bfloat16)
        ag_copy(b, 1, 0).start()
        ag_copy(b, 0, 1).start()
        ag_copy(b, 1, 1).start()
        ag_copy(b, 0, 0).start()
        for h in range(2):
            own_store(b, h).start()

    def hand_on(b):
        for s in (1, 0):
            ag_copy(b, s, 0 if s == 1 else 1).wait_recv()
            fwd_copy(b, s).start()
            fwd_store(b, s).start()

    def step(b, carry):
        attention(b)

        @pl.when(b >= 1)
        def _():
            pass_on(b - 1)

        @pl.when(b >= 2)
        def _():
            finish(b - 2)

        @pl.when(b >= 3)
        def _():
            hand_on(b - 3)

        project(b)
        return carry

    lax.fori_loop(0, BLOCKS, step, 0)
    last = BLOCKS - 1
    pass_on(last)
    finish(last - 1)
    hand_on(last - 2)
    hand_on(last - 1)
    finish(last)
    hand_on(last)

    def drain(b, carry):
        for s in range(2):
            opp_copy(b, s).wait_send()
            fwd_copy(b, s).wait()
            fwd_store(b, s).wait()
            for h in range(2):
                side_copy(b, s, h).wait_send()
                ag_copy(b, s, h).wait_send()
            ag_copy(b, s, 1 if s == 1 else 0).wait_recv()
        for h in range(2):
            own_store(b, h).wait()
        return carry

    lax.fori_loop(0, BLOCKS, drain, 0)


def mix(n, q, k, v, pos_q, pos_k, hidden, w_out):
    heads, rows, _ = q.shape
    seq = k.shape[0]
    width = hidden.shape[1]
    half = width // n // 2
    blk = rows // BLOCKS
    bf16, f32 = jnp.bfloat16, jnp.float32
    dma = pltpu.SemaphoreType.DMA
    vmem = pl.BlockSpec(memory_space=pltpu.VMEM)
    hbm = pl.BlockSpec(memory_space=pl.ANY)
    return pl.pallas_call(
        functools.partial(mix_kernel, n),
        out_shape=jax.ShapeDtypeStruct((rows, width), bf16),
        in_specs=[vmem] * 5 + [hbm] * 2,
        out_specs=hbm,
        scratch_shapes=[
            pltpu.VMEM((2 * n, w_out.shape[0], half), bf16),
            pltpu.VMEM((rows, 2 * half), bf16),
            pltpu.VMEM((blk, seq), f32),
            pltpu.VMEM((blk, heads * HEAD), bf16),
            pltpu.VMEM((BLOCKS, 2, blk, half), bf16),
            pltpu.VMEM((BLOCKS, 2, blk, half), bf16),
            pltpu.VMEM((BLOCKS, 2, 2, blk, half), bf16),
            pltpu.VMEM((BLOCKS, 2, 2, blk, half), bf16),
            pltpu.VMEM((BLOCKS, 2, blk, half), f32),
            pltpu.VMEM((BLOCKS, 2, blk, half), f32),
            pltpu.VMEM((BLOCKS, 2, blk, half), bf16),
            pltpu.VMEM((BLOCKS, 2, blk, half), bf16),
            dma((2 * n,)),
            dma,
            dma((BLOCKS, 4)),
            dma((BLOCKS, 2)),
            dma((BLOCKS, 2)),
            dma((BLOCKS, 2, 2)),
            dma((BLOCKS, 2, 2)),
            dma((BLOCKS, 2, 2)),
            dma((BLOCKS, 2, 2)),
            dma((BLOCKS, 2)),
            dma((BLOCKS, 2)),
        ],
        compiler_params=pltpu.CompilerParams(collective_id=0, has_side_effects=True, vmem_limit_bytes=60 * 1024 * 1024),
    )(q, k, v, pos_q, pos_k, hidden, w_out)


def solution(mesh):
    n = mesh.shape["tp"]

    def local_block(hidden, tok_pos, norm_gain, w_query, w_key, w_value, w_out):
        rows, width = hidden.shape
        heads_loc = w_query.shape[1] // HEAD
        kv_loc = w_key.shape[1] // HEAD
        normed = rms_normed(hidden.astype(jnp.float32), norm_gain)
        cos_tab, sin_tab = rope_tables(tok_pos)
        keys_raw = jnp.dot(normed, w_key, preferred_element_type=jnp.float32).astype(jnp.bfloat16).reshape(rows, kv_loc, HEAD)
        k_rot = rotate_half(keys_raw, cos_tab, sin_tab)
        values = jnp.dot(normed, w_value, preferred_element_type=jnp.float32).astype(jnp.bfloat16)
        k_all = lax.all_gather(k_rot.reshape(rows, kv_loc * HEAD), "cp", axis=0, tiled=True)
        v_all = lax.all_gather(values, "cp", axis=0, tiled=True)
        pos_all = lax.all_gather(tok_pos, "cp", axis=0, tiled=True)
        queries = jnp.dot(normed, w_query, preferred_element_type=jnp.float32).astype(jnp.bfloat16).reshape(rows, heads_loc, HEAD)
        q_rot = rotate_half(queries, cos_tab, sin_tab).transpose(1, 0, 2)
        hidden_out = mix(n, q_rot, k_all, v_all, tok_pos[:, None], pos_all[None, :], hidden, w_out)
        return hidden_out, k_rot, values.reshape(rows, kv_loc, HEAD)

    row_spec = P(("dp", "cp"), None)
    cache_spec = P(("dp", "cp"), "tp", None)
    return jax.shard_map(local_block, mesh=mesh, in_specs=(row_spec, P(("dp", "cp")), P(None), P(None, "tp"), P(None, "tp"), P(None, "tp"), P("tp", None)), out_specs=(row_spec, cache_spec, cache_spec), check_vma=False)
```

```python
import functools
import math

import jax
import jax.numpy as jnp
from jax import lax
from jax.experimental import pallas as pl
from jax.experimental.pallas import tpu as pltpu
from jax.sharding import PartitionSpec as P

HEAD = 128
THETA = 1000000
EPS = 1e-5
MESH = pl.DeviceIdType.MESH
BLOCKS = 4
STACK = 4
SLAB = 256
SLOTS = 8
OPP, PREV, NEXT, OWN = 0, 1, 2, 3
W_ORDER = (2 * OPP, 2 * OPP + 1, 2 * PREV + 1, 2 * NEXT, 2 * PREV, 2 * NEXT + 1, 2 * OWN, 2 * OWN + 1)


def rope_tables(tok_pos):
    inv_freq = 1.0 / (THETA ** (jnp.arange(0, HEAD, 2, dtype=jnp.float32) / HEAD))
    angles = tok_pos.astype(jnp.float32)[:, None] * inv_freq[None, :]
    cos, sin = jnp.cos(angles), jnp.sin(angles)
    return jnp.concatenate([cos, cos], axis=-1), jnp.concatenate([-sin, sin], axis=-1)


def block_kernel(
    n, shards,
    gain_ref, cos_ref, sin_ref, posq_ref, posrow_ref, x_hbm, wq_hbm, wk_hbm, wv_hbm, wo_hbm,
    out_hbm, k_hbm, v_hbm,
    h_ref, w_ref, q_ref, kv_ref, posk_ref, x_ref, bias_ref, o_ref,
    opp_send, opp_recv, side_send, side_recv, side_part, own_part, own_out, fwd_recv,
    h_sem, w_sem, x_sem, cache_sem, kv_ssem, kv_rsem, pos_ssem, pos_rsem,
    out_sem, opp_ssem, opp_rsem, side_ssem, side_rsem, ag_ssem, ag_rsem, fwd_ssem, fwd_rsem,
):
    heads, rows, _ = q_ref.shape
    seq = shards * rows
    width = h_ref.shape[1]
    kv_heads = wk_hbm.shape[1] // HEAD
    q_per_kv = heads // kv_heads
    stack = min(STACK, q_per_kv)
    q_tiles = heads * HEAD // SLAB
    deep = heads * HEAD
    chunk = width // n
    half = chunk // 2
    subs = half // SLAB
    blk = rows // BLOCKS
    coef = HEAD ** -0.5 * math.log2(math.e)

    me = lax.axis_index("tp")
    right, left = lax.rem(me + 1, n), lax.rem(me + n - 1, n)
    owners = (lax.rem(me + 2, n), left, right, me)
    spot = lax.axis_index("cp")
    chips = shards // 2
    core, chip = lax.rem(spot, 2), spot // 2
    mate = chip * 2 + 1 - core
    ahead = lax.rem(chip + 1, chips) * 2 + core
    behind = lax.rem(chip + chips - 1, chips) * 2 + core
    across = lax.rem(chip + 2, chips) * 2 + core
    slot_of = lambda t: (t % SLOTS) if isinstance(t, int) else lax.rem(t, SLOTS)

    def h_copy(c):
        part = pl.ds(c * (rows // 4), rows // 4)
        return pltpu.make_async_copy(x_hbm.at[part], h_ref.at[part], h_sem.at[c])

    def slab_copy(ref, col, t):
        return pltpu.make_async_copy(ref.at[:, pl.ds(col, SLAB)], w_ref.at[slot_of(t)], w_sem.at[slot_of(t)])

    def q_slab(j):
        return slab_copy(wq_hbm, pl.multiple_of(j * SLAB, SLAB), 2 + j)

    def wo_copy(p, sub):
        idx = W_ORDER[p]
        col = pl.multiple_of(owners[idx // 2] * chunk + (idx % 2) * half + sub * SLAB, SLAB)
        slot = slot_of(2 + p)
        return pltpu.make_async_copy(wo_hbm.at[:, pl.ds(col, SLAB)], w_ref.at[slot, pl.ds(sub * deep, deep)], w_sem.at[slot])

    def start_wo(p):
        for sub in range(subs):
            wo_copy(p, sub).start()

    def wait_wo(p):
        slot = slot_of(2 + p)
        both = w_ref.at[slot, pl.ds(0, subs * deep)]
        pltpu.make_async_copy(both, both, w_sem.at[slot]).wait()

    x_copy = pltpu.make_async_copy(x_hbm.at[:, pl.ds(pl.multiple_of(me * chunk, chunk), chunk)], x_ref, x_sem)

    for c in range(4):
        h_copy(c).start()
    slab_copy(wk_hbm, 0, 0).start()
    slab_copy(wv_hbm, 0, 1).start()
    early = min(q_tiles, SLOTS - 2)
    for j in range(early):
        q_slab(j).start()

    barrier = pltpu.get_barrier_semaphore()
    for side in (left, right):
        pl.semaphore_signal(barrier, inc=1, device_id={"tp": side}, device_id_type=MESH)
    for d in range(1, shards):
        pl.semaphore_signal(barrier, inc=1, device_id={"cp": lax.rem(spot + d, shards)}, device_id_type=MESH)
    pl.semaphore_wait(barrier, 1 + shards)

    def pos_copy(d):
        return pltpu.make_async_remote_copy(
            src_ref=posrow_ref, dst_ref=posk_ref.at[spot], send_sem=pos_ssem.at[d], recv_sem=pos_rsem.at[spot],
            device_id={"cp": lax.rem(spot + d, shards)}, device_id_type=MESH)

    def pos_arrival(d):
        source = lax.rem(spot + d, shards)
        return pltpu.make_async_remote_copy(
            src_ref=posrow_ref, dst_ref=posk_ref.at[source], send_sem=pos_ssem.at[d], recv_sem=pos_rsem.at[source],
            device_id={"cp": source}, device_id_type=MESH)

    for d in range(1, shards):
        pos_copy(d).start()
    posk_ref[spot] = posrow_ref[...]

    def kv_copy(kind, owner, to, s):
        return pltpu.make_async_remote_copy(
            src_ref=kv_ref.at[kind, owner], dst_ref=kv_ref.at[kind, owner], send_sem=kv_ssem.at[kind, s],
            recv_sem=kv_rsem.at[kind, owner], device_id={"cp": to}, device_id_type=MESH)

    def cache_copy(kind):
        return pltpu.make_async_copy(kv_ref.at[kind, spot], (k_hbm, v_hbm)[kind], cache_sem.at[kind])

    def kv_first(kind):
        kv_copy(kind, spot, ahead, 0).start()
        kv_copy(kind, spot, behind, 1).start()
        kv_copy(kind, spot, mate, 2).start()
        cache_copy(kind).start()

    def kv_relay(kind):
        source, to = ((behind, ahead), (ahead, behind))[kind]
        kv_copy(kind, source, to, 3).wait_recv()
        kv_copy(kind, source, to, 3).start()
        kv_copy(kind, source, mate, 4).start()

    def kv_rest(kind):
        source = (ahead, behind)[kind]
        kv_copy(kind, source, mate, 5).wait_recv()
        kv_copy(kind, source, mate, 5).start()

    def kv_last(kind):
        kv_copy(kind, across, mate, 6).wait_recv()
        kv_copy(kind, across, mate, 6).start()

    def kv_mate(kind):
        for owner in (spot, ahead, behind, across):
            twin = (owner // 2) * 2 + 1 - core
            kv_copy(kind, twin, mate, 2).wait_recv()

    piece = min(width, 1024)
    group = 16 if rows // 4 >= 16 else rows // 4
    for c in range(4):
        h_copy(c).wait()

        def norm_step(g, carry, c=c):
            row = pl.ds(pl.multiple_of(c * (rows // 4) + g * group, group), group)
            acc = jnp.zeros((group, piece), jnp.float32)
            for p in range(width // piece):
                x = h_ref[row, p * piece:(p + 1) * piece].astype(jnp.float32)
                acc = acc + x * x
            scale = lax.rsqrt(jnp.sum(acc, axis=-1, keepdims=True) * (1.0 / width) + EPS)
            for p in range(width // piece):
                cols = slice(p * piece, (p + 1) * piece)
                x = h_ref[row, cols].astype(jnp.float32)
                h_ref[row, cols] = (x * scale * gain_ref[:, cols]).astype(jnp.bfloat16)
            return carry

        lax.fori_loop(0, rows // 4 // group, norm_step, 0)

    def rotated(u):
        u = u.astype(jnp.bfloat16).astype(jnp.float32)
        return (u * cos_ref[...] + pltpu.roll(u, HEAD // 2, 1) * sin_ref[...]).astype(jnp.bfloat16)

    def qkv_step(t, carry):
        slab_copy(wq_hbm, 0, t).wait()
        res = jnp.dot(h_ref[...], w_ref[slot_of(t)], preferred_element_type=jnp.float32)

        @pl.when(t == 0)
        def _():
            for h in range(SLAB // HEAD):
                kv_ref[0, spot, :, h * HEAD:(h + 1) * HEAD] = rotated(res[:, h * HEAD:(h + 1) * HEAD])
            kv_first(0)

        @pl.when(t == 1)
        def _():
            kv_ref[1, spot] = res.astype(jnp.bfloat16)
            kv_first(1)

        @pl.when(t >= 2)
        def _():
            for h in range(SLAB // HEAD):
                q_ref[(t - 2) * (SLAB // HEAD) + h] = rotated(res[:, h * HEAD:(h + 1) * HEAD])

        for j in range(early, q_tiles):
            @pl.when(t == j + 2 - SLOTS)
            def _(j=j):
                q_slab(j).start()
        for p in range(2 * n):
            if p < q_tiles:
                @pl.when(t == 2 + p)
                def _(p=p):
                    start_wo(p)

        @pl.when(t == q_tiles // 2 + 1)
        def _():
            kv_relay(0)

        @pl.when(t == q_tiles)
        def _():
            kv_relay(1)

        return carry

    lax.fori_loop(0, 2 + q_tiles, qkv_step, 0)
    for p in range(q_tiles, 2 * n):
        start_wo(p)
    x_copy.start()
    kv_rest(0)
    kv_rest(1)
    kv_last(0)
    kv_last(1)
    for d in range(1, shards):
        pos_arrival(d).wait_recv()
    kv_mate(0)
    kv_mate(1)

    sides = (left, right)

    def opp_copy(b, s):
        return pltpu.make_async_remote_copy(
            src_ref=opp_send.at[b, s], dst_ref=opp_recv.at[b, s], send_sem=opp_ssem.at[b, s], recv_sem=opp_rsem.at[b, s],
            device_id={"tp": sides[s]}, device_id_type=MESH)

    def side_copy(b, s, h):
        return pltpu.make_async_remote_copy(
            src_ref=side_send.at[b, s, h], dst_ref=side_recv.at[b, s, h], send_sem=side_ssem.at[b, s, h],
            recv_sem=side_rsem.at[b, s, h], device_id={"tp": sides[s]}, device_id_type=MESH)

    def out_at(b, owner, h):
        row = pl.multiple_of(b * blk, blk)
        col = pl.multiple_of(owner * chunk + h * half, half)
        return out_hbm.at[pl.ds(row, blk), pl.ds(col, half)]

    def ag_copy(b, s, h):
        hands_on = h == (0 if s == 1 else 1)
        dst = fwd_recv.at[b, s] if hands_on else out_at(b, me, h)
        return pltpu.make_async_remote_copy(
            src_ref=own_out.at[b, h], dst_ref=dst, send_sem=ag_ssem.at[b, s, h], recv_sem=ag_rsem.at[b, s, h],
            device_id={"tp": sides[s]}, device_id_type=MESH)

    def fwd_copy(b, s):
        owner, h = (left, 0) if s == 1 else (right, 1)
        return pltpu.make_async_remote_copy(
            src_ref=fwd_recv.at[b, s], dst_ref=out_at(b, owner, h), send_sem=fwd_ssem.at[b, s], recv_sem=fwd_rsem.at[b, s],
            device_id={"tp": sides[s]}, device_id_type=MESH)

    def own_store(b, h):
        return pltpu.make_async_copy(own_out.at[b, h], out_at(b, me, h), out_sem.at[b, h])

    def fwd_store(b, s):
        owner, h = (left, 0) if s == 1 else (right, 1)
        return pltpu.make_async_copy(fwd_recv.at[b, s], out_at(b, owner, h), out_sem.at[b, 2 + s])

    def attention(b):
        row = pl.multiple_of(b * blk, blk)
        for i in range(shards):
            bias_ref[:, i * rows:(i + 1) * rows] = jnp.where(posk_ref[i] <= posq_ref[pl.ds(row, blk), :], 0.0, -jnp.inf)

        def heads_step(i, carry):
            first = i * stack
            kv = pl.multiple_of((first // q_per_kv) * HEAD, HEAD)
            q = q_ref[pl.ds(first, stack), pl.ds(row, blk), :].reshape(stack * blk, HEAD)
            k = kv_ref[0, :, :, pl.ds(kv, HEAD)].reshape(seq, HEAD)
            v = kv_ref[1, :, :, pl.ds(kv, HEAD)].reshape(seq, HEAD)
            s = lax.dot_general(q, k, (((1,), (1,)), ((), ())), preferred_element_type=jnp.float32)
            s = (s * coef).reshape(stack, blk, seq) + bias_ref[...][None]
            s = s.reshape(stack * blk, seq)
            p = jnp.exp2(s - jnp.max(s, axis=-1, keepdims=True))
            total = jnp.sum(p, axis=-1, keepdims=True)
            o = jnp.dot(p.astype(jnp.bfloat16), v, preferred_element_type=jnp.float32)
            o = (o / total).astype(jnp.bfloat16)
            for h in range(stack):
                o_ref[:, pl.ds(pl.multiple_of((first + h) * HEAD, HEAD), HEAD)] = o[h * blk:(h + 1) * blk]
            return carry

        lax.fori_loop(0, heads // stack, heads_step, 0)

    def project(b):
        def part(p, dst, dtype):
            @pl.when(b == 0)
            def _():
                wait_wo(p)
            for sub in range(subs):
                w = w_ref[slot_of(2 + p), sub * deep:(sub + 1) * deep, :]
                res = jnp.dot(o_ref[...], w, preferred_element_type=jnp.float32)
                dst[:, sub * SLAB:(sub + 1) * SLAB] = res.astype(dtype)

        bf16, f32 = jnp.bfloat16, jnp.float32
        part(0, opp_send.at[b, 0], bf16)
        opp_copy(b, 0).start()
        part(1, opp_send.at[b, 1], bf16)
        opp_copy(b, 1).start()
        part(2, side_send.at[b, 0, 1], bf16)
        side_copy(b, 0, 1).start()
        part(3, side_send.at[b, 1, 0], bf16)
        side_copy(b, 1, 0).start()
        part(4, side_part.at[b, 0], f32)
        part(5, side_part.at[b, 1], f32)
        for h in range(2):
            part(6 + h, own_part.at[b, h], f32)

    def pass_on(b):
        for s in range(2):
            opp_copy(b, s).wait_recv()
            side_send[b, s, s] = (side_part[b, s] + opp_recv[b, s].astype(jnp.float32)).astype(jnp.bfloat16)
            side_copy(b, s, s).start()

    def finish(b):
        row = pl.multiple_of(b * blk, blk)

        @pl.when(b == 0)
        def _():
            x_copy.wait()

        for h in range(2):
            for s in range(2):
                side_copy(b, s, h).wait_recv()
            total = own_part[b, h] + side_recv[b, 0, h].astype(jnp.float32) + side_recv[b, 1, h].astype(jnp.float32)
            x = x_ref[pl.ds(row, blk), h * half:(h + 1) * half].astype(jnp.float32)
            own_out[b, h] = (x + total).astype(jnp.bfloat16)
        ag_copy(b, 1, 0).start()
        ag_copy(b, 0, 1).start()
        ag_copy(b, 1, 1).start()
        ag_copy(b, 0, 0).start()
        for h in range(2):
            own_store(b, h).start()

    def hand_on(b):
        for s in (1, 0):
            ag_copy(b, s, 0 if s == 1 else 1).wait_recv()
            fwd_copy(b, s).start()
            fwd_store(b, s).start()

    def step(b, carry):
        attention(b)

        @pl.when(b >= 1)
        def _():
            pass_on(b - 1)

        @pl.when(b >= 2)
        def _():
            finish(b - 2)

        @pl.when(b >= 3)
        def _():
            hand_on(b - 3)

        project(b)
        return carry

    lax.fori_loop(0, BLOCKS, step, 0)
    last = BLOCKS - 1
    pass_on(last)
    finish(last - 1)
    hand_on(last - 2)
    hand_on(last - 1)
    finish(last)
    hand_on(last)

    def drain(b, carry):
        for s in range(2):
            opp_copy(b, s).wait_send()
            fwd_copy(b, s).wait()
            fwd_store(b, s).wait()
            for h in range(2):
                side_copy(b, s, h).wait_send()
                ag_copy(b, s, h).wait_send()
            ag_copy(b, s, 1 if s == 1 else 0).wait_recv()
        for h in range(2):
            own_store(b, h).wait()
        return carry

    lax.fori_loop(0, BLOCKS, drain, 0)
    for d in range(1, shards):
        pos_copy(d).wait_send()
    for kind in range(2):
        cache_copy(kind).wait()
        for s in range(7):
            kv_copy(kind, spot, mate, s).wait_send()


def block_call(n, shards, gain, cos, sin, tok_pos, hidden, w_query, w_key, w_value, w_out):
    rows, width = hidden.shape
    heads = w_query.shape[1] // HEAD
    kv_cols = w_key.shape[1]
    half = width // n // 2
    blk = rows // BLOCKS
    bf16, f32 = jnp.bfloat16, jnp.float32
    dma = pltpu.SemaphoreType.DMA
    vmem = pl.BlockSpec(memory_space=pltpu.VMEM)
    hbm = pl.BlockSpec(memory_space=pl.ANY)
    return pl.pallas_call(
        functools.partial(block_kernel, n, shards),
        out_shape=(
            jax.ShapeDtypeStruct((rows, width), bf16),
            jax.ShapeDtypeStruct((rows, kv_cols), bf16),
            jax.ShapeDtypeStruct((rows, kv_cols), bf16),
        ),
        in_specs=[vmem] * 5 + [hbm] * 5,
        out_specs=(hbm, hbm, hbm),
        scratch_shapes=[
            pltpu.VMEM((rows, width), bf16),
            pltpu.VMEM((SLOTS, width, SLAB), bf16),
            pltpu.VMEM((heads, rows, HEAD), bf16),
            pltpu.VMEM((2, shards, rows, kv_cols), bf16),
            pltpu.VMEM((shards, 1, rows), jnp.int32),
            pltpu.VMEM((rows, 2 * half), bf16),
            pltpu.VMEM((blk, shards * rows), f32),
            pltpu.VMEM((blk, heads * HEAD), bf16),
            pltpu.VMEM((BLOCKS, 2, blk, half), bf16),
            pltpu.VMEM((BLOCKS, 2, blk, half), bf16),
            pltpu.VMEM((BLOCKS, 2, 2, blk, half), bf16),
            pltpu.VMEM((BLOCKS, 2, 2, blk, half), bf16),
            pltpu.VMEM((BLOCKS, 2, blk, half), f32),
            pltpu.VMEM((BLOCKS, 2, blk, half), f32),
            pltpu.VMEM((BLOCKS, 2, blk, half), bf16),
            pltpu.VMEM((BLOCKS, 2, blk, half), bf16),
            dma((4,)),
            dma((SLOTS,)),
            dma,
            dma((2,)),
            dma((2, 7)),
            dma((2, shards)),
            dma((shards,)),
            dma((shards,)),
            dma((BLOCKS, 4)),
            dma((BLOCKS, 2)),
            dma((BLOCKS, 2)),
            dma((BLOCKS, 2, 2)),
            dma((BLOCKS, 2, 2)),
            dma((BLOCKS, 2, 2)),
            dma((BLOCKS, 2, 2)),
            dma((BLOCKS, 2)),
            dma((BLOCKS, 2)),
        ],
        compiler_params=pltpu.CompilerParams(collective_id=0, has_side_effects=True, vmem_limit_bytes=60 * 1024 * 1024),
    )(gain, cos, sin, tok_pos[:, None], tok_pos[None, :], hidden, w_query, w_key, w_value, w_out)


def solution(mesh):
    n, shards = mesh.shape["tp"], mesh.shape["cp"]

    def local_block(hidden, tok_pos, norm_gain, w_query, w_key, w_value, w_out):
        rows = hidden.shape[0]
        kv_loc = w_key.shape[1] // HEAD
        cos, sin = rope_tables(tok_pos)
        hidden_out, k_rot, values = block_call(n, shards, norm_gain[None, :], cos, sin, tok_pos, hidden, w_query, w_key, w_value, w_out)
        return hidden_out, k_rot.reshape(rows, kv_loc, HEAD), values.reshape(rows, kv_loc, HEAD)

    row_spec = P(("dp", "cp"), None)
    cache_spec = P(("dp", "cp"), "tp", None)
    return jax.shard_map(local_block, mesh=mesh, in_specs=(row_spec, P(("dp", "cp")), P(None), P(None, "tp"), P(None, "tp"), P(None, "tp"), P("tp", None)), out_specs=(row_spec, cache_spec, cache_spec), check_vma=False)
```

```python
import functools
import math

import jax
import jax.numpy as jnp
import numpy as np
from jax import lax
from jax.experimental import pallas as pl
from jax.experimental.pallas import tpu as pltpu
from jax.sharding import PartitionSpec as P

HEAD = 128
THETA = 1000000
EPS = 1e-5
MESH = pl.DeviceIdType.MESH
BLOCKS = 4
STACK = 4
SLAB = 256
SLOTS = 6
OPP, PREV, NEXT, OWN = 0, 1, 2, 3
W_ORDER = (2 * OPP, 2 * OPP + 1, 2 * PREV + 1, 2 * NEXT, 2 * PREV, 2 * NEXT + 1, 2 * OWN, 2 * OWN + 1)


def inv_freqs():
    freqs = 1.0 / THETA ** (np.arange(0, HEAD, 2, dtype=np.float64) / HEAD)
    return np.concatenate([freqs, freqs])[None, :].astype(np.float32)


def block_kernel(
    n, shards,
    gain_ref, freq_ref, posrow_ref, x_hbm, wq_hbm, wk_hbm, wv_hbm, wo_hbm,
    out_hbm, k_hbm, v_hbm,
    h_ref, w_ref, wkv_ref, q_ref, kv_ref, posk_ref, cos_ref, sin_ref, x_ref, bias_ref, o_ref,
    opp_send, opp_recv, side_send, side_recv, side_part, own_part, own_out, fwd_recv,
    h_sem, w_sem, wkv_sem, x_sem, cache_sem, kv_ssem, kv_rsem, pos_ssem, pos_rsem,
    out_sem, opp_ssem, opp_rsem, side_ssem, side_rsem, ag_ssem, ag_rsem, fwd_ssem, fwd_rsem,
):
    heads, rows, _ = q_ref.shape
    seq = shards * rows
    width = h_ref.shape[1]
    kv_heads = wk_hbm.shape[1] // HEAD
    q_per_kv = heads // kv_heads
    stack = min(STACK, q_per_kv)
    deep = heads * HEAD
    chunk = width // n
    half = chunk // 2
    subs = half // SLAB
    depths = width // deep
    q_tiles = depths * (deep // half)
    blk = rows // BLOCKS
    coef = HEAD ** -0.5 * math.log2(math.e)

    me = lax.axis_index("tp")
    right, left = lax.rem(me + 1, n), lax.rem(me + n - 1, n)
    owners = (lax.rem(me + 2, n), left, right, me)
    spot = lax.axis_index("cp")
    chips = shards // 2
    core, chip = lax.rem(spot, 2), spot // 2
    mate = chip * 2 + 1 - core
    ahead = lax.rem(chip + 1, chips) * 2 + core
    behind = lax.rem(chip + chips - 1, chips) * 2 + core
    across = lax.rem(chip + 2, chips) * 2 + core
    def h_copy(c):
        part = pl.ds(c * (rows // 4), rows // 4)
        return pltpu.make_async_copy(x_hbm.at[part], h_ref.at[part], h_sem.at[c])

    def kv_tile(kind):
        return pltpu.make_async_copy((wk_hbm, wv_hbm)[kind], wkv_ref.at[kind], wkv_sem.at[kind])

    def q_tile(t, slot):
        row, col = (t % depths) * deep, (t // depths) * half
        return pltpu.make_async_copy(wq_hbm.at[pl.ds(row, deep), pl.ds(col, half)], w_ref.at[slot], w_sem.at[slot])

    wo_slots = [(q_tiles - SLOTS + p) % SLOTS for p in range(2 * n - 2)]

    def wo_copies(p):
        idx = W_ORDER[p]
        col = owners[idx // 2] * chunk + (idx % 2) * half
        if p < 2 * n - 2:
            src = wo_hbm.at[:, pl.ds(pl.multiple_of(col, half), half)]
            return [pltpu.make_async_copy(src, w_ref.at[wo_slots[p]], w_sem.at[wo_slots[p]])]
        kind = p - (2 * n - 2)
        return [
            pltpu.make_async_copy(
                wo_hbm.at[:, pl.ds(pl.multiple_of(col + sub * SLAB, SLAB), SLAB)],
                wkv_ref.at[kind, pl.ds(sub * deep, deep)], wkv_sem.at[kind])
            for sub in range(subs)
        ]

    def start_wo(p):
        for copy in wo_copies(p):
            copy.start()

    def wait_wo(p):
        if p < 2 * n - 2:
            wo_copies(p)[0].wait()
        else:
            whole = wkv_ref.at[p - (2 * n - 2), pl.ds(0, subs * deep)]
            pltpu.make_async_copy(whole, whole, wkv_sem.at[p - (2 * n - 2)]).wait()

    x_copy = pltpu.make_async_copy(x_hbm.at[:, pl.ds(pl.multiple_of(me * chunk, chunk), chunk)], x_ref, x_sem)

    for c in range(4):
        h_copy(c).start()
    kv_tile(0).start()
    kv_tile(1).start()
    for t in range(SLOTS):
        q_tile(t, t).start()

    barrier = pltpu.get_barrier_semaphore()
    for side in (left, right):
        pl.semaphore_signal(barrier, inc=1, device_id={"tp": side}, device_id_type=MESH)
    for d in range(1, shards):
        pl.semaphore_signal(barrier, inc=1, device_id={"cp": lax.rem(spot + d, shards)}, device_id_type=MESH)
    pl.semaphore_wait(barrier, 1 + shards)

    def pos_copy(d):
        return pltpu.make_async_remote_copy(
            src_ref=posrow_ref, dst_ref=posk_ref.at[spot], send_sem=pos_ssem.at[d], recv_sem=pos_rsem.at[spot],
            device_id={"cp": lax.rem(spot + d, shards)}, device_id_type=MESH)

    def pos_arrival(d):
        source = lax.rem(spot + d, shards)
        return pltpu.make_async_remote_copy(
            src_ref=posrow_ref, dst_ref=posk_ref.at[source], send_sem=pos_ssem.at[d], recv_sem=pos_rsem.at[source],
            device_id={"cp": source}, device_id_type=MESH)

    for d in range(1, shards):
        pos_copy(d).start()
    posk_ref[spot] = posrow_ref[...]

    def kv_copy(kind, owner, to, s):
        return pltpu.make_async_remote_copy(
            src_ref=kv_ref.at[kind, owner], dst_ref=kv_ref.at[kind, owner], send_sem=kv_ssem.at[kind, s],
            recv_sem=kv_rsem.at[kind, owner], device_id={"cp": to}, device_id_type=MESH)

    def cache_copy(kind):
        return pltpu.make_async_copy(kv_ref.at[kind, spot], (k_hbm, v_hbm)[kind], cache_sem.at[kind])

    def kv_first(kind):
        kv_copy(kind, spot, ahead, 0).start()
        kv_copy(kind, spot, behind, 1).start()
        kv_copy(kind, spot, mate, 2).start()
        cache_copy(kind).start()

    def kv_relay(kind):
        source, to = ((behind, ahead), (ahead, behind))[kind]
        kv_copy(kind, source, to, 3).wait_recv()
        kv_copy(kind, source, to, 3).start()
        kv_copy(kind, source, mate, 4).start()

    def kv_rest(kind):
        source = (ahead, behind)[kind]
        kv_copy(kind, source, mate, 5).wait_recv()
        kv_copy(kind, source, mate, 5).start()

    def kv_last(kind):
        kv_copy(kind, across, mate, 6).wait_recv()
        kv_copy(kind, across, mate, 6).start()

    def kv_mate(kind):
        for owner in (spot, ahead, behind, across):
            twin = (owner // 2) * 2 + 1 - core
            kv_copy(kind, twin, mate, 2).wait_recv()

    piece = min(width, 1024)
    group = 16 if rows // 4 >= 16 else rows // 4
    for c in range(4):
        h_copy(c).wait()

        def norm_step(g, carry, c=c):
            row = pl.ds(pl.multiple_of(c * (rows // 4) + g * group, group), group)
            acc = jnp.zeros((group, piece), jnp.float32)
            for p in range(width // piece):
                x = h_ref[row, p * piece:(p + 1) * piece].astype(jnp.float32)
                acc = acc + x * x
            scale = lax.rsqrt(jnp.sum(acc, axis=-1, keepdims=True) * (1.0 / width) + EPS)
            for p in range(width // piece):
                cols = slice(p * piece, (p + 1) * piece)
                x = h_ref[row, cols].astype(jnp.float32)
                h_ref[row, cols] = (x * scale * gain_ref[:, cols]).astype(jnp.bfloat16)
            return carry

        lax.fori_loop(0, rows // 4 // group, norm_step, 0)

    def rotated(u):
        u = u.astype(jnp.bfloat16).astype(jnp.float32)
        return (u * cos_ref[...] + pltpu.roll(u, HEAD // 2, 1) * sin_ref[...]).astype(jnp.bfloat16)

    def column(row, size):
        own = posrow_ref[...].astype(jnp.float32)
        hit = lax.broadcasted_iota(jnp.int32, (size, rows), 0) + row == lax.broadcasted_iota(jnp.int32, (size, rows), 1)
        return jnp.sum(jnp.where(hit, own, 0.0), axis=-1, keepdims=True)

    for c in range(4):
        part = slice(c * (rows // 4), (c + 1) * (rows // 4))
        angle = column(c * (rows // 4), rows // 4) * freq_ref[...]
        sin = jnp.sin(angle)
        cos_ref[part] = jnp.cos(angle)
        sin_ref[part] = jnp.where(lax.broadcasted_iota(jnp.int32, angle.shape, 1) < HEAD // 2, -sin, sin)

    def kv_step(kind, carry):
        for k in range(2):
            @pl.when(kind == k)
            def _(k=k):
                kv_tile(k).wait()
        res = jnp.dot(h_ref[...], wkv_ref[kind], preferred_element_type=jnp.float32)

        @pl.when(kind == 0)
        def _():
            for h in range(kv_heads):
                kv_ref[0, spot, :, h * HEAD:(h + 1) * HEAD] = rotated(res[:, h * HEAD:(h + 1) * HEAD])
            kv_first(0)

        @pl.when(kind == 1)
        def _():
            kv_ref[1, spot] = res.astype(jnp.bfloat16)
            kv_first(1)

        return carry

    lax.fori_loop(0, 2, kv_step, 0)

    def q_step(t, carry):
        slot = lax.rem(t, SLOTS)
        depth, side = lax.rem(t, depths), t // depths
        pltpu.make_async_copy(w_ref.at[slot], w_ref.at[slot], w_sem.at[slot]).wait()
        res = jnp.dot(
            h_ref[:, pl.ds(pl.multiple_of(depth * deep, deep), deep)], w_ref[slot], preferred_element_type=jnp.float32
        ).reshape(BLOCKS, blk, half)

        @pl.when(depth == 0)
        def _():
            side_part[:, 0] = res

        @pl.when(jnp.logical_and(depth > 0, depth < depths - 1))
        def _():
            side_part[:, 0] += res

        @pl.when(depth == depths - 1)
        def _():
            for h in range(half // HEAD):
                cols = slice(h * HEAD, (h + 1) * HEAD)
                full = (side_part[:, 0, :, cols] + res[:, :, cols]).reshape(rows, HEAD)
                q_ref[side * (half // HEAD) + h] = rotated(full)

        for j in range(SLOTS, q_tiles):
            @pl.when(t == j - SLOTS)
            def _(j=j):
                q_tile(j, j % SLOTS).start()
        for p in range(2 * n - 2):
            @pl.when(t == q_tiles - SLOTS + p)
            def _(p=p):
                start_wo(p)

        @pl.when(t == q_tiles // 2 - 1)
        def _():
            kv_relay(0)

        @pl.when(t == q_tiles - 2)
        def _():
            kv_relay(1)

        return carry

    lax.fori_loop(0, q_tiles, q_step, 0)
    for p in range(2 * n - 2, 2 * n):
        start_wo(p)
    x_copy.start()
    kv_rest(0)
    kv_rest(1)
    kv_last(0)
    kv_last(1)
    for d in range(1, shards):
        pos_arrival(d).wait_recv()
    kv_mate(0)
    kv_mate(1)

    sides = (left, right)

    def opp_copy(b, s):
        return pltpu.make_async_remote_copy(
            src_ref=opp_send.at[b, s], dst_ref=opp_recv.at[b, s], send_sem=opp_ssem.at[b, s], recv_sem=opp_rsem.at[b, s],
            device_id={"tp": sides[s]}, device_id_type=MESH)

    def side_copy(b, s, h):
        return pltpu.make_async_remote_copy(
            src_ref=side_send.at[b, s, h], dst_ref=side_recv.at[b, s, h], send_sem=side_ssem.at[b, s, h],
            recv_sem=side_rsem.at[b, s, h], device_id={"tp": sides[s]}, device_id_type=MESH)

    def out_at(b, owner, h):
        row = pl.multiple_of(b * blk, blk)
        col = pl.multiple_of(owner * chunk + h * half, half)
        return out_hbm.at[pl.ds(row, blk), pl.ds(col, half)]

    def ag_copy(b, s, h):
        hands_on = h == (0 if s == 1 else 1)
        dst = fwd_recv.at[b, s] if hands_on else out_at(b, me, h)
        return pltpu.make_async_remote_copy(
            src_ref=own_out.at[b, h], dst_ref=dst, send_sem=ag_ssem.at[b, s, h], recv_sem=ag_rsem.at[b, s, h],
            device_id={"tp": sides[s]}, device_id_type=MESH)

    def fwd_copy(b, s):
        owner, h = (left, 0) if s == 1 else (right, 1)
        return pltpu.make_async_remote_copy(
            src_ref=fwd_recv.at[b, s], dst_ref=out_at(b, owner, h), send_sem=fwd_ssem.at[b, s], recv_sem=fwd_rsem.at[b, s],
            device_id={"tp": sides[s]}, device_id_type=MESH)

    def own_store(b, h):
        return pltpu.make_async_copy(own_out.at[b, h], out_at(b, me, h), out_sem.at[b, h])

    def fwd_store(b, s):
        owner, h = (left, 0) if s == 1 else (right, 1)
        return pltpu.make_async_copy(fwd_recv.at[b, s], out_at(b, owner, h), out_sem.at[b, 2 + s])

    def attention(b):
        row = pl.multiple_of(b * blk, blk)
        own = column(row, blk)
        for i in range(shards):
            bias_ref[:, i * rows:(i + 1) * rows] = jnp.where(posk_ref[i].astype(jnp.float32) <= own, 0.0, -jnp.inf)

        def heads_step(i, carry):
            first = i * stack
            kv = pl.multiple_of((first // q_per_kv) * HEAD, HEAD)
            q = q_ref[pl.ds(first, stack), pl.ds(row, blk), :].reshape(stack * blk, HEAD)
            k = kv_ref[0, :, :, pl.ds(kv, HEAD)].reshape(seq, HEAD)
            v = kv_ref[1, :, :, pl.ds(kv, HEAD)].reshape(seq, HEAD)
            s = lax.dot_general(q, k, (((1,), (1,)), ((), ())), preferred_element_type=jnp.float32)
            s = (s * coef).reshape(stack, blk, seq) + bias_ref[...][None]
            s = s.reshape(stack * blk, seq)
            p = jnp.exp2(s - jnp.max(s, axis=-1, keepdims=True))
            total = jnp.sum(p, axis=-1, keepdims=True)
            o = jnp.dot(p.astype(jnp.bfloat16), v, preferred_element_type=jnp.float32)
            o = (o / total).astype(jnp.bfloat16)
            for h in range(stack):
                o_ref[:, pl.ds(pl.multiple_of((first + h) * HEAD, HEAD), HEAD)] = o[h * blk:(h + 1) * blk]
            return carry

        lax.fori_loop(0, heads // stack, heads_step, 0)

    def project(b):
        def part(p, dst, dtype):
            @pl.when(b == 0)
            def _():
                wait_wo(p)
            if p < 2 * n - 2:
                dst[...] = jnp.dot(o_ref[...], w_ref[wo_slots[p]], preferred_element_type=jnp.float32).astype(dtype)
            else:
                for sub in range(subs):
                    w = wkv_ref[p - (2 * n - 2), sub * deep:(sub + 1) * deep, :]
                    res = jnp.dot(o_ref[...], w, preferred_element_type=jnp.float32)
                    dst[:, sub * SLAB:(sub + 1) * SLAB] = res.astype(dtype)

        bf16, f32 = jnp.bfloat16, jnp.float32
        part(0, opp_send.at[b, 0], bf16)
        opp_copy(b, 0).start()
        part(1, opp_send.at[b, 1], bf16)
        opp_copy(b, 1).start()
        part(2, side_send.at[b, 0, 1], bf16)
        side_copy(b, 0, 1).start()
        part(3, side_send.at[b, 1, 0], bf16)
        side_copy(b, 1, 0).start()
        part(4, side_part.at[b, 0], f32)
        part(5, side_part.at[b, 1], f32)
        for h in range(2):
            part(6 + h, own_part.at[b, h], f32)

    def pass_on(b):
        for s in range(2):
            opp_copy(b, s).wait_recv()
            side_send[b, s, s] = (side_part[b, s] + opp_recv[b, s].astype(jnp.float32)).astype(jnp.bfloat16)
            side_copy(b, s, s).start()

    def finish(b):
        row = pl.multiple_of(b * blk, blk)

        @pl.when(b == 0)
        def _():
            x_copy.wait()

        for h in range(2):
            for s in range(2):
                side_copy(b, s, h).wait_recv()
            total = own_part[b, h] + side_recv[b, 0, h].astype(jnp.float32) + side_recv[b, 1, h].astype(jnp.float32)
            x = x_ref[pl.ds(row, blk), h * half:(h + 1) * half].astype(jnp.float32)
            own_out[b, h] = (x + total).astype(jnp.bfloat16)
        ag_copy(b, 1, 0).start()
        ag_copy(b, 0, 1).start()
        ag_copy(b, 1, 1).start()
        ag_copy(b, 0, 0).start()
        for h in range(2):
            own_store(b, h).start()

    def hand_on(b):
        for s in (1, 0):
            ag_copy(b, s, 0 if s == 1 else 1).wait_recv()
            fwd_copy(b, s).start()
            fwd_store(b, s).start()

    def step(b, carry):
        attention(b)

        @pl.when(b >= 1)
        def _():
            pass_on(b - 1)

        @pl.when(b >= 2)
        def _():
            finish(b - 2)

        @pl.when(b >= 3)
        def _():
            hand_on(b - 3)

        project(b)
        return carry

    lax.fori_loop(0, BLOCKS, step, 0)
    last = BLOCKS - 1
    pass_on(last)
    finish(last - 1)
    hand_on(last - 2)
    hand_on(last - 1)
    finish(last)
    hand_on(last)

    def drain(b, carry):
        for s in range(2):
            opp_copy(b, s).wait_send()
            fwd_copy(b, s).wait()
            fwd_store(b, s).wait()
            for h in range(2):
                side_copy(b, s, h).wait_send()
                ag_copy(b, s, h).wait_send()
            ag_copy(b, s, 1 if s == 1 else 0).wait_recv()
        for h in range(2):
            own_store(b, h).wait()
        return carry

    lax.fori_loop(0, BLOCKS, drain, 0)
    for d in range(1, shards):
        pos_copy(d).wait_send()
    for kind in range(2):
        cache_copy(kind).wait()
        for s in range(7):
            kv_copy(kind, spot, mate, s).wait_send()


def tidy_kernel(out_hbm, k_ref, v_ref, res_hbm, k_out, v_out, buf, in_sem, out_sem):
    pieces, size = buf.shape[:2]

    def load(i):
        return pltpu.make_async_copy(out_hbm.at[pl.ds(i * size, size)], buf.at[i], in_sem.at[i])

    def store(i):
        return pltpu.make_async_copy(buf.at[i], res_hbm.at[pl.ds(i * size, size)], out_sem.at[i])

    for i in range(pieces):
        load(i).start()
    for src, dst in ((k_ref, k_out), (v_ref, v_out)):
        for h in range(dst.shape[1]):
            dst[:, h, :] = src[:, h * HEAD:(h + 1) * HEAD]
    for i in range(pieces):
        load(i).wait()
        store(i).start()
    for i in range(pieces):
        store(i).wait()


def tidy_call(out, k, v):
    rows, width = out.shape
    heads = k.shape[1] // HEAD
    pieces = 8
    vmem = pl.BlockSpec(memory_space=pltpu.VMEM)
    hbm = pl.BlockSpec(memory_space=pl.ANY)
    cache = jax.ShapeDtypeStruct((rows, heads, HEAD), k.dtype)
    return pl.pallas_call(
        tidy_kernel,
        out_shape=(jax.ShapeDtypeStruct(out.shape, out.dtype), cache, cache),
        in_specs=[hbm, vmem, vmem],
        out_specs=(hbm, vmem, vmem),
        scratch_shapes=[
            pltpu.VMEM((pieces, rows // pieces, width), out.dtype),
            pltpu.SemaphoreType.DMA((pieces,)),
            pltpu.SemaphoreType.DMA((pieces,)),
        ],
        compiler_params=pltpu.CompilerParams(vmem_limit_bytes=60 * 1024 * 1024),
    )(out, k, v)


def block_call(n, shards, gain, tok_pos, hidden, w_query, w_key, w_value, w_out):
    rows, width = hidden.shape
    heads = w_query.shape[1] // HEAD
    kv_cols = w_key.shape[1]
    half = width // n // 2
    blk = rows // BLOCKS
    bf16, f32 = jnp.bfloat16, jnp.float32
    dma = pltpu.SemaphoreType.DMA
    vmem = pl.BlockSpec(memory_space=pltpu.VMEM)
    hbm = pl.BlockSpec(memory_space=pl.ANY)
    return pl.pallas_call(
        functools.partial(block_kernel, n, shards),
        out_shape=(
            jax.ShapeDtypeStruct((rows, width), bf16),
            jax.ShapeDtypeStruct((rows, kv_cols), bf16),
            jax.ShapeDtypeStruct((rows, kv_cols), bf16),
        ),
        in_specs=[vmem] * 3 + [hbm] * 5,
        out_specs=(hbm, hbm, hbm),
        scratch_shapes=[
            pltpu.VMEM((rows, width), bf16),
            pltpu.VMEM((SLOTS, w_out.shape[0], half), bf16),
            pltpu.VMEM((2, width, kv_cols), bf16),
            pltpu.VMEM((heads, rows, HEAD), bf16),
            pltpu.VMEM((2, shards, rows, kv_cols), bf16),
            pltpu.VMEM((shards, 1, rows), jnp.int32),
            pltpu.VMEM((rows, HEAD), f32),
            pltpu.VMEM((rows, HEAD), f32),
            pltpu.VMEM((rows, 2 * half), bf16),
            pltpu.VMEM((blk, shards * rows), f32),
            pltpu.VMEM((blk, heads * HEAD), bf16),
            pltpu.VMEM((BLOCKS, 2, blk, half), bf16),
            pltpu.VMEM((BLOCKS, 2, blk, half), bf16),
            pltpu.VMEM((BLOCKS, 2, 2, blk, half), bf16),
            pltpu.VMEM((BLOCKS, 2, 2, blk, half), bf16),
            pltpu.VMEM((BLOCKS, 2, blk, half), f32),
            pltpu.VMEM((BLOCKS, 2, blk, half), f32),
            pltpu.VMEM((BLOCKS, 2, blk, half), bf16),
            pltpu.VMEM((BLOCKS, 2, blk, half), bf16),
            dma((4,)),
            dma((SLOTS,)),
            dma((2,)),
            dma,
            dma((2,)),
            dma((2, 7)),
            dma((2, shards)),
            dma((shards,)),
            dma((shards,)),
            dma((BLOCKS, 4)),
            dma((BLOCKS, 2)),
            dma((BLOCKS, 2)),
            dma((BLOCKS, 2, 2)),
            dma((BLOCKS, 2, 2)),
            dma((BLOCKS, 2, 2)),
            dma((BLOCKS, 2, 2)),
            dma((BLOCKS, 2)),
            dma((BLOCKS, 2)),
        ],
        compiler_params=pltpu.CompilerParams(collective_id=0, has_side_effects=True, vmem_limit_bytes=60 * 1024 * 1024),
    )(gain, jnp.asarray(inv_freqs()), tok_pos[None, :], hidden, w_query, w_key, w_value, w_out)


def solution(mesh):
    n, shards = mesh.shape["tp"], mesh.shape["cp"]

    def local_block(hidden, tok_pos, norm_gain, w_query, w_key, w_value, w_out):
        return tidy_call(*block_call(n, shards, norm_gain[None, :], tok_pos, hidden, w_query, w_key, w_value, w_out))

    row_spec = P(("dp", "cp"), None)
    cache_spec = P(("dp", "cp"), "tp", None)
    return jax.shard_map(local_block, mesh=mesh, in_specs=(row_spec, P(("dp", "cp")), P(None), P(None, "tp"), P(None, "tp"), P(None, "tp"), P("tp", None)), out_specs=(row_spec, cache_spec, cache_spec), check_vma=False)
```
